32 devices in a mesh: dp: 1 (over z), sp: 32 (over x, y, core).
Axes of the slice: x: 4, y: 4, z: 1, core: 2. Of those that a mesh axis runs over, the one named last changes fastest.
The devices are a block of a 4x4x8 slice.
Arguments:
- x: bfloat16 [4096, 4096], P(('dp', 'sp'))
- gain: bfloat16 [4096], replicated
- wq: bfloat16 [4096, 4096], replicated
- wk: bfloat16 [4096, 256], replicated
- wv: bfloat16 [4096, 256], replicated
- wo: bfloat16 [4096, 4096], replicated
Outputs:
- output: bfloat16 [4096, 4096], P(('dp', 'sp'))
All inputs are finite; a program needn't handle non-finite values.
Results may differ from the reference program's by a relative error of at most 0.012.
Values are sent between devices in bfloat16 or wider.
A program may use at most 768 MiB of HBM per device.

```python
import jax
import jax.numpy as jnp
from jax import lax

ROWS = 4096
D = 4096
HEADS = 32
KV_HEADS = 2
HEAD = 128
THETA = 10000


def setup_inputs(seed: int = 0, part: int = 0) -> dict:
    kx, kn, kq, kk, kv, ko = jax.random.split(jax.random.key(seed), 6)

    def weights(key, rows, columns):
        return jax.random.normal(key, (rows, columns), jnp.float32) * rows**-0.5

    drawn = {
        "x": jax.random.normal(jax.random.fold_in(kx, part), (ROWS, D), jnp.float32),
        "gain": 1 + 0.1 * jax.random.normal(kn, (D,), jnp.float32),
        "wq": 2 * weights(kq, D, HEADS * HEAD),
        "wk": 2 * weights(kk, D, KV_HEADS * HEAD),
        "wv": 4 * weights(kv, D, KV_HEADS * HEAD),
        "wo": weights(ko, HEADS * HEAD, D),
    }
    return {k: v.astype(jnp.bfloat16) for k, v in drawn.items()}


def normed(x, gain):
    wide = x.astype(jnp.float32)
    scale = lax.rsqrt(jnp.mean(wide * wide, -1, keepdims=True) + 1e-6)
    return (wide * scale * gain.astype(jnp.float32)).astype(jnp.bfloat16)


def turned(t, place, theta):
    half = t.shape[-1] // 2
    angle = place.astype(jnp.float32)[:, None] * theta ** (-jnp.arange(half, dtype=jnp.float32) / half)
    cos, sin = jnp.cos(angle)[:, None], jnp.sin(angle)[:, None]
    a, b = t[..., :half].astype(jnp.float32), t[..., half:].astype(jnp.float32)
    return jnp.concatenate([a * cos - b * sin, b * cos + a * sin], -1).astype(jnp.bfloat16)


def matmul(a, w):
    return jnp.dot(a, w, preferred_element_type=jnp.float32).astype(jnp.bfloat16)


def einsum(form, a, b):
    return jnp.einsum(form, a.astype(jnp.float32), b.astype(jnp.float32))


def attention(q, k, v):
    scores = einsum("tgsd,ugd->gstu", q, k) * q.shape[-1] ** -0.5
    token = jnp.arange(q.shape[0])
    scores = jnp.where(token[:, None] >= token, scores, -jnp.inf)
    weights = jax.nn.softmax(scores, -1).astype(jnp.bfloat16)
    return einsum("gstu,ugd->tgsd", weights, v).astype(jnp.bfloat16)


def reference(x, gain, wq, wk, wv, wo):
    a, place = normed(x, gain), jnp.arange(ROWS)
    q = turned(matmul(a, wq).reshape(ROWS, HEADS, HEAD), place, THETA).reshape(ROWS, KV_HEADS, -1, HEAD)
    k = turned(matmul(a, wk).reshape(ROWS, KV_HEADS, HEAD), place, THETA)
    v = matmul(a, wv).reshape(ROWS, KV_HEADS, HEAD)
    seen = attention(q, k, v).reshape(ROWS, HEADS * HEAD)
    return (x.astype(jnp.float32) + jnp.dot(seen, wo, preferred_element_type=jnp.float32)).astype(jnp.bfloat16)
```

```python
import functools
import math

import jax
import jax.numpy as jnp
from jax import lax
from jax.experimental import pallas as pl
from jax.experimental.pallas import tpu as pltpu
from jax.sharding import PartitionSpec as P

HEAD = 128
THETA = 10000
NEG = -1e30
HIDDEN = 2 * NEG
LOG2E = 1.4426950408889634
VMEM = 63 * 2**20
PAIR = 2
PARTS = 4
QCOLS = 256
OCOLS = 512
WIDE = 512
EXTRA = 16


def _dot(a, b, ca, cb):
    return lax.dot_general(a, b, (((ca,), (cb,)), ((), ())), preferred_element_type=jnp.float32)


def _kernel(side, x_hbm, gain_ref, cos_ref, sin_ref, wq_hbm, wk_hbm, wv_hbm, wo_hbm, y_hbm,
            x_s, a_s, wk_s, wv_s, wq_s, wo_s, q_s, k_s, v_s, top_s, mix_s, seen_s, part_s, came_s, y_s,
            x_sem, wk_sem, wv_sem, wq_sem, wo_sem, y_sem, a_send, a_recv, k_recv, v_recv, k1_send, k2_send, vx_send, vy_send, v2_send,
            p_send, p_recv):
    me = lax.axis_index("sp")
    n, c = me // PAIR, me % PAIR
    row, col = n // side, n % side
    own = x_s.shape[0]
    toks = PAIR * own
    heads = q_s.shape[0]
    cols = heads * toks
    width = wq_s.shape[0] * QCOLS
    e = HEAD**-0.5 * LOG2E

    def dev(r, q, core):
        return {"sp": (r * side + q) * PAIR + core}

    mate = dev(row, col, 1 - c)

    x_copy = pltpu.make_async_copy(x_hbm, x_s, x_sem)
    x_copy.start()
    head_cols = pl.ds(pl.multiple_of(c * HEAD, HEAD), HEAD)
    wk_copy = pltpu.make_async_copy(wk_hbm.at[:, head_cols], wk_s, wk_sem)
    wv_copy = pltpu.make_async_copy(wv_hbm.at[:, head_cols], wv_s, wv_sem)
    wk_copy.start()
    wv_copy.start()

    def wq_copy(j):
        at = pl.ds(pl.multiple_of(c * width + j * QCOLS, QCOLS), QCOLS)
        return pltpu.make_async_copy(wq_hbm.at[:, at], wq_s.at[j], wq_sem.at[j])

    def wo_copy(j):
        rows = pl.ds(pl.multiple_of(c * width, QCOLS), width)
        return pltpu.make_async_copy(wo_hbm.at[rows, pl.ds(pl.multiple_of(j * OCOLS, OCOLS), OCOLS)], wo_s.at[j], wo_sem.at[j])

    nq, no = wq_s.shape[0], wo_s.shape[0]
    for j in range(nq):
        wq_copy(j).start()

    barrier = pltpu.get_barrier_semaphore()
    pl.semaphore_signal(barrier, inc=1, device_id=mate, device_id_type=pl.DeviceIdType.MESH)
    for d in range(1, side):
        pl.semaphore_signal(barrier, inc=1, device_id=dev(row, (col + d) % side, c), device_id_type=pl.DeviceIdType.MESH)
        pl.semaphore_signal(barrier, inc=1, device_id=dev((row + d) % side, col, c), device_id_type=pl.DeviceIdType.MESH)

    x_copy.wait()
    step = own // PARTS
    for p in range(PARTS):
        wide = x_s[p * step : (p + 1) * step, :].astype(jnp.float32)
        scale = lax.rsqrt(jnp.mean(wide * wide, -1, keepdims=True) + 1e-6)
        at = pl.ds(pl.multiple_of(c * own + p * step, step), step)
        a_s[at, :] = (wide * scale * gain_ref[...].astype(jnp.float32)).astype(jnp.bfloat16)
    pl.semaphore_wait(barrier, 2 * side - 1)

    def a_copy(p):
        at = pl.ds(pl.multiple_of(c * own + p * step, step), step)
        return pltpu.make_async_remote_copy(a_s.at[at, :], a_s.at[at, :], a_send.at[p], a_recv.at[p], device_id=mate,
                                            device_id_type=pl.DeviceIdType.MESH)

    for p in range(PARTS):
        a_copy(p).start()
    v_s[:, HEAD:, :] = jnp.ones((v_s.shape[0], EXTRA, toks), jnp.bfloat16)
    wk_copy.wait()
    wv_copy.wait()
    for p in range(PARTS):
        a_copy(p).wait_recv()

    def turned(t):
        return (t * cos_ref[...] + pltpu.roll(t, HEAD // 2, 1) * sin_ref[...]).astype(jnp.bfloat16)

    a = a_s[...]
    k = _dot(a, wk_s[...], 1, 0).astype(jnp.bfloat16).astype(jnp.float32)
    k_s[n] = turned(k)
    v = _dot(a, wv_s[...], 1, 0)
    v_s[n, :HEAD, :] = v.T.astype(jnp.bfloat16)

    def k_copy(block, r, q, sem):
        return pltpu.make_async_remote_copy(k_s.at[block], k_s.at[block], sem, k_recv.at[block], device_id=dev(r, q, c),
                                            device_id_type=pl.DeviceIdType.MESH)

    def v_copy(block, r, q, sem):
        return pltpu.make_async_remote_copy(v_s.at[block, pl.ds(0, HEAD)], v_s.at[block, pl.ds(0, HEAD)], sem, v_recv.at[block],
                                            device_id=dev(r, q, c), device_id_type=pl.DeviceIdType.MESH)

    def each_first(do):
        for d in (1, side - 1, *range(2, side - 1)):
            q = (col + d) % side
            do(k_copy(n, row, q, k1_send.at[d]))
            r = (row + d) % side

            @pl.when(r > row)
            def _():
                do(v_copy(n, r, col, vx_send.at[d]))

            @pl.when(q > col)
            def _():
                do(v_copy(n, row, q, vy_send.at[d]))

    def each_k_second(do):
        for r in range(side - 1, 0, -1):

            @pl.when(r > row)
            def _():
                for q in range(side):
                    do(k_copy(row * side + q, r, col, k2_send.at[r, q]))

    def each_v_second(do):
        for r in range(side - 2, -1, -1):

            @pl.when(r < row)
            def _():
                for d in (1, side - 1, *range(2, side - 1)):
                    do(v_copy(r * side + col, row, (col + d) % side, v2_send.at[r, d]))

    def k_wait(block):
        k_copy(block, row, (col + 1) % side, k1_send.at[1]).wait_recv()

    def v_wait(block):
        v_copy(block, row, (col + 1) % side, vx_send.at[1]).wait_recv()

    each_first(lambda copy: copy.start())

    def queries(j):
        wq_copy(j).wait()
        got = _dot(a_s[...], wq_s[j], 1, 0).astype(jnp.bfloat16).astype(jnp.float32)
        for i in range(QCOLS // HEAD):
            q_s[j * (QCOLS // HEAD) + i] = turned(got[:, i * HEAD : (i + 1) * HEAD])

    def first_queries(j, _):
        queries(j)
        wo_copy(j).start()

    lax.fori_loop(0, nq, first_queries, None)

    for d in range(1, side):
        k_wait(row * side + (col + d) % side)
    each_k_second(lambda copy: copy.start())
    for r in range(side - 1):

        @pl.when(r < row)
        def _():
            v_wait(r * side + col)

    each_v_second(lambda copy: copy.start())

    per = WIDE // toks

    def attend(blocks, masked, first):
        keys = jnp.concatenate([k_s[b] for b in blocks], axis=0)
        values = jnp.concatenate([v_s[b] for b in blocks], axis=1)
        size = len(blocks) * toks
        if masked:
            gap = lax.broadcasted_iota(jnp.int32, (size, toks), 1) - lax.broadcasted_iota(jnp.int32, (size, toks), 0)
            ok = jnp.concatenate([gap >= 0] * per, axis=1)
        for i in range(heads // per):
            here = slice(i * WIDE, (i + 1) * WIDE)
            s = _dot(keys, q_s[i * per : (i + 1) * per].reshape(WIDE, HEAD), 1, 1)
            if masked:
                s = jnp.where(ok, s, HIDDEN)
            top = s.max(axis=0, keepdims=True)
            if not first:
                old = top_s[:, here]
                top = jnp.maximum(old, top)
            top_s[:, here] = top
            p = jnp.exp2((s - top) * e).astype(jnp.bfloat16)
            more = _dot(values, p, 1, 0)
            mix_s[:, here] = more if first else mix_s[:, here] * jnp.exp2((old - top) * e) + more

    attend([n], True, True)

    def beside(d, _):
        b = row * side + d
        v_wait(b)
        attend([b], False, False)

    lax.fori_loop(0, col, beside, None)

    def before(t, _):
        r, half = row - 1 - t // 2, t % 2
        b = r * side + 2 * half
        for i in range(2):
            k_wait(b + i)

            @pl.when(b + i != r * side + col)
            def _():
                v_wait(b + i)

        attend([b, b + 1], False, False)

    lax.fori_loop(0, 2 * row, before, None)

    for h in range(heads):
        here = slice(h * toks, (h + 1) * toks)
        out = mix_s[:HEAD, here] * (1 / mix_s[HEAD : HEAD + 1, here])
        seen_s[:, h * HEAD : (h + 1) * HEAD] = out.T.astype(jnp.bfloat16)

    mine = pl.ds(pl.multiple_of(c * own, own), own)
    theirs = pl.ds(pl.multiple_of((1 - c) * own, own), own)

    def p_copy(j):
        return pltpu.make_async_remote_copy(part_s.at[j, theirs], came_s.at[j], p_send.at[j], p_recv.at[j], device_id=mate,
                                            device_id_type=pl.DeviceIdType.MESH)

    def y_copy(j):
        return pltpu.make_async_copy(y_s.at[j], y_hbm.at[:, pl.ds(pl.multiple_of(j * OCOLS, OCOLS), OCOLS)], y_sem.at[j])

    def finish(j):
        p_copy(j).wait_recv()
        wide = x_s[:, pl.ds(pl.multiple_of(j * OCOLS, OCOLS), OCOLS)].astype(jnp.float32)
        y_s[j] = (wide + (part_s[j, mine] + came_s[j])).astype(jnp.bfloat16)
        y_copy(j).start()

    lag = 2

    def project(j, _):
        wo_copy(j).wait()
        part_s[j] = _dot(seen_s[...], wo_s[j], 1, 0)
        p_copy(j).start()

        @pl.when(j >= lag)
        def _():
            finish(j - lag)

    lax.fori_loop(0, no, project, None)
    for j in range(no - lag, no):
        finish(j)

    for p in range(PARTS):
        a_copy(p).wait_send()
    each_first(lambda copy: copy.wait_send())
    each_k_second(lambda copy: copy.wait_send())
    each_v_second(lambda copy: copy.wait_send())
    for j in range(no):
        p_copy(j).wait_send()
        y_copy(j).wait()


def solution(mesh):
    chips = mesh.shape["sp"] // PAIR
    side = math.isqrt(chips)

    def step(x, gain, wq, wk, wv, wo):
        own, d = x.shape
        toks = PAIR * own
        half = HEAD // 2
        width = wq.shape[1] // PAIR
        heads = width // HEAD
        place = (lax.axis_index("sp") // PAIR) * toks + jnp.arange(toks)
        angle = place.astype(jnp.float32)[:, None] * THETA ** (-jnp.arange(half, dtype=jnp.float32) / half)
        cos, sin = jnp.cos(angle), jnp.sin(angle)
        cos, sin = jnp.concatenate([cos, cos], -1), jnp.concatenate([-sin, sin], -1)
        nq, no = width // QCOLS, d // OCOLS
        bf, f32 = jnp.bfloat16, jnp.float32
        dma = pltpu.SemaphoreType.DMA
        anywhere, vmem = pl.BlockSpec(memory_space=pl.ANY), pl.BlockSpec(memory_space=pltpu.VMEM)
        return pl.pallas_call(
            functools.partial(_kernel, side),
            out_shape=jax.ShapeDtypeStruct((own, d), bf),
            in_specs=[anywhere, vmem, vmem, vmem, anywhere, anywhere, anywhere, anywhere],
            out_specs=anywhere,
            scratch_shapes=[
                pltpu.VMEM((own, d), bf),
                pltpu.VMEM((toks, d), bf),
                pltpu.VMEM((d, HEAD), bf),
                pltpu.VMEM((d, HEAD), bf),
                pltpu.VMEM((nq, d, QCOLS), bf),
                pltpu.VMEM((no, width, OCOLS), bf),
                pltpu.VMEM((heads, toks, HEAD), bf),
                pltpu.VMEM((chips, toks, HEAD), bf),
                pltpu.VMEM((chips, HEAD + EXTRA, toks), bf),
                pltpu.VMEM((1, heads * toks), f32),
                pltpu.VMEM((HEAD + EXTRA, heads * toks), f32),
                pltpu.VMEM((toks, width), bf),
                pltpu.VMEM((no, toks, OCOLS), f32),
                pltpu.VMEM((no, own, OCOLS), f32),
                pltpu.VMEM((no, own, OCOLS), bf),
                dma, dma, dma, dma((nq,)), dma((no,)), dma((no,)),
                dma((PARTS,)), dma((PARTS,)), dma((chips,)), dma((chips,)),
                dma((side,)), dma((side, side)), dma((side,)), dma((side,)), dma((side, side)),
                dma((no,)), dma((no,)),
            ],
            compiler_params=pltpu.CompilerParams(collective_id=0, has_side_effects=True, vmem_limit_bytes=VMEM),
        )(x, gain[None], cos, sin, wq, wk, wv, wo)

    tokens, whole = P(("dp", "sp"), None), P(None, None)
    return jax.shard_map(
        step,
        mesh=mesh,
        in_specs=(tokens, P(None), whole, whole, whole, whole),
        out_specs=tokens,
        check_vma=False,
    )
```
